256 devices in a mesh: expert: 16 (over x, y), dp: 16 (over z, core).
Axes of the slice: x: 4, y: 4, z: 8, core: 2. Of those that a mesh axis runs over, the one named last changes fastest.
Arguments:
- tokens: bfloat16 [2, 32768, 1280], P(None, ('expert', 'dp')), may hold values from -6 to 6
- modality: int32 [2, 32768], P(None, ('expert', 'dp')), may hold values from 0 to 1, as said below
- routes: int32 [2, 32768, 1], P(None, ('expert', 'dp')), may hold values from 0 to 15; in each aligned block of 128 rows (0 to 127, 128 to 255, ..., all dimensions but the last counted through in order) at most 16 rows name the same one
- router: bfloat16 [1280, 16], replicated, may hold values from -0.15625 to 0.15625
- w_in: bfloat16 [16, 1280, 5120], P('expert', 'dp'), may hold values from -0.15625 to 0.15625
- w_out: bfloat16 [16, 5120, 1280], P('expert', 'dp'), may hold values from -0.078125 to 0.078125
Outputs:
- mixed: bfloat16 [2, 32768, 1280], P(None, ('expert', 'dp'))
- load: float32 [2, 2, 16], replicated
The draws below stay inside these ranges and needn't reach their ends.
Inputs may be any that keep to these rules, and one draw needn't show every extreme that they name: `routes`: among the 128 tokens of one micro-batch on one device (aligned blocks of 128 rows), at most 16 are routed to any one expert. `modality`: in every aligned block of 128 tokens of a micro-batch, the number of text tokens lies between 32 and 96.
All inputs are finite; a program needn't handle non-finite values.
Results may differ from the reference program's by a relative error of at most 0.0057.
Values may be sent and summed in bfloat16 or wider, within the bound.
No kernel may reach another device: no remote copies, remote signals or barrier semaphores. Data moves between devices by JAX's collectives and lax.ppermute only.
A program may use at most 192 MiB of HBM per device.

```python
import math
import jax
import jax.numpy as jnp
import numpy as np
from jax import lax

D = 1280
FF = 5120
MB = 2
TOK_MB = 128
EXPERTS = 16
CAP = 16
TOKENS = 32768


def draw_modality(key, part):
    n_blocks = TOKENS // TOK_MB
    scores = jax.random.randint(key, (MB, n_blocks, TOK_MB), 0, 1 << 20) * TOK_MB + jnp.arange(TOK_MB, dtype=jnp.int32)
    order = jnp.argsort(scores, axis=-1)
    ranked = jnp.argsort(order, axis=-1)
    texts = TOK_MB // 4 + TOK_MB // 2 * jnp.arange(n_blocks, dtype=jnp.int32) // max(n_blocks - 1, 1)
    return (ranked < texts[None, :, None]).astype(jnp.int32).reshape(MB, TOKENS)


def level_of(key, shape, cuts, least, largest):
    def one(axis_at, shards_of):
        heights = jax.random.uniform(jax.random.fold_in(jax.random.fold_in(key, 6), axis_at), (shards_of,), jnp.float32, least / len(cuts), largest / len(cuts))
        return jnp.repeat(jnp.exp(heights), shape[axis_at] // shards_of).reshape((-1,) + (1,) * (len(shape) - axis_at - 1))

    gain = one(*cuts[0])
    for cut in cuts[1:]:
        gain = gain * one(*cut)
    return gain


def shared_out(key, own, number, rows, count, top, reach, skew):
    order = jax.random.permutation(key, count)
    crowded, common = load_shares(count, rows * top, reach, skew, True), load_shares(count, rows * top, reach, skew, False)
    places = jnp.arange(count)

    def named(sizes, offset_by):
        used = int((sizes > 0).sum())
        fixed = max(1, used // 4)
        shifted = fixed + (places - fixed + offset_by * (used - fixed)) % max(1, count - fixed)
        return jnp.zeros((count,), jnp.int32).at[order[jnp.where(places < fixed, places, shifted)]].set(jnp.asarray(sizes, jnp.int32))

    sizes = jnp.where(number % 4 == 0, named(crowded, number // 4), named(common, number - number // 4 - 1))
    mixed = jax.random.permutation(jax.random.fold_in(own, 3), count)
    donor, sink = mixed[0:count // 2 * 2:2], mixed[1:count // 2 * 2:2]
    room = jnp.minimum(sizes[donor] - 1, reach - sizes[sink]) // 2
    room = jnp.where((donor == order[0]) | (sink == order[0]) | (sizes[sink] == 0), 0, jnp.maximum(room, 0))
    shifted = jax.random.randint(jax.random.fold_in(own, 4), (count // 2,), 0, 1 << 20) % (room + 1)
    sizes = sizes.at[donor].add(-shifted).at[sink].add(shifted)
    items = jnp.searchsorted(jnp.cumsum(sizes), jnp.arange(rows * top), side="right").astype(jnp.int32)
    listing = items.reshape(top, rows).T
    listing = listing[jax.random.permutation(jax.random.fold_in(own, 1), rows)]
    offset_by = jax.random.randint(jax.random.fold_in(own, 2), (rows, 1), 0, top)
    return jnp.take_along_axis(listing, (jnp.arange(top)[None, :] + offset_by) % top, axis=1)


def load_shares(number_of, total, most, skew, full):
    portions = [(1 << 20) // math.isqrt(grade ** skew) + 1 for grade in range(1, number_of + 1)]
    largest = most if full else min(most, max(-(-total // number_of), total * portions[0] // sum(portions)))
    least = 1 if total - largest >= number_of - 1 else 0
    given, rest = [largest] + [least] * (number_of - 1), total - largest - least * (number_of - 1)
    while rest > 0:
        candidates = [i for i in range(1, number_of) if given[i] < largest] or [i for i in range(1, number_of) if given[i] < most]
        pool, budget = sum([portions[i] for i in candidates]), rest
        for i in candidates:
            extra = min(most - given[i], max(1, budget * portions[i] // pool), rest)
            given[i] = given[i] + extra
            rest = rest - extra
    return np.array(given)


def gaussian(stream_key, shape, deviation, reach, pieces=(), kind=jnp.bfloat16):
    drawn = jax.random.normal(stream_key, shape, jnp.float32) * deviation
    if len(pieces) > 0:
        drawn = level_of(stream_key, shape, pieces, -0.22, 0.18) * drawn
    return jnp.clip(drawn, min=-reach, max=reach).astype(kind)


def setup_inputs(seed: int = 0) -> dict:
    streams_of = jax.random.split(jax.random.key(seed), 7)
    tokens = gaussian(streams_of[0], (MB, TOKENS, D), 1.0, 6.0, ((1, 256),))
    modality = draw_modality(jax.random.fold_in(streams_of[6], 71), 0)
    routes_keys = jax.random.split(jax.random.fold_in(streams_of[2], 1), MB * TOKENS // TOK_MB)
    routes_turns = jax.random.permutation(jax.random.fold_in(streams_of[2], 3), MB * TOKENS // TOK_MB)
    routes = jax.vmap(lambda own, number: shared_out(jax.random.fold_in(streams_of[2], 2), own, number, TOK_MB, EXPERTS, 1, CAP, 2))(routes_keys, routes_turns).reshape((MB, TOKENS, 1))
    router = gaussian(streams_of[3], (D, EXPERTS), D ** -0.5, 0.15625)
    w_in = gaussian(streams_of[4], (EXPERTS, D, FF), D ** -0.5, 0.15625, ((0, 16), (1, 16)))
    w_out = gaussian(streams_of[5], (EXPERTS, FF, D), FF ** -0.5, 0.078125, ((0, 16), (1, 16)))
    return dict(tokens=tokens, modality=modality, routes=routes, router=router, w_in=w_in, w_out=w_out)


def expert_mlp(operands):
    rows_in, weight_in, weight_out = operands
    pre_act = jnp.dot(rows_in, weight_in, preferred_element_type=jnp.float32)
    hidden = jax.nn.gelu(pre_act, approximate=True).astype(jnp.bfloat16)
    return jnp.dot(hidden, weight_out, preferred_element_type=jnp.float32).astype(jnp.bfloat16)


def reference(tokens, modality, routes, router, w_in, w_out):
    blocks = TOKENS // TOK_MB
    slot_bound = blocks * CAP
    mixed_list = []
    counts = jnp.zeros((2, EXPERTS), jnp.float32)
    prob_sums = jnp.zeros((2, EXPERTS), jnp.float32)
    modal_counts = jnp.zeros((2,), jnp.float32)
    for micro in range(MB):
        micro_tokens = tokens[micro]
        expert_ids = routes[micro, :, 0].astype(jnp.int32)
        logits = jnp.dot(micro_tokens, router, preferred_element_type=jnp.float32)
        onehot = (expert_ids[:, None] == jnp.arange(EXPERTS, dtype=jnp.int32)[None, :]).astype(jnp.float32)
        gating = jax.nn.sigmoid(jnp.sum(logits * onehot, axis=-1))
        running = jnp.cumsum(onehot.reshape(blocks, TOK_MB, EXPERTS), axis=1).reshape(TOKENS, EXPERTS)
        slot_pos = (jnp.sum(running * onehot, axis=-1) - 1.0).astype(jnp.int32)
        device = (jnp.arange(TOKENS, dtype=jnp.int32) // TOK_MB).astype(jnp.int32)
        position = (expert_ids * slot_bound + device * CAP + slot_pos).astype(jnp.int32)
        buffer = jnp.zeros((EXPERTS * slot_bound, D), jnp.bfloat16).at[position].set(micro_tokens)
        buffer = buffer.reshape(EXPERTS, slot_bound, D)
        result = lax.map(expert_mlp, (buffer, w_in, w_out)).reshape(EXPERTS * slot_bound, D)
        scaled = result[position].astype(jnp.float32) * gating[:, None]
        mixed_list.append(scaled.astype(jnp.bfloat16))
        exps = jnp.exp(logits)
        router_probs = exps / jnp.sum(exps, axis=-1, keepdims=True)
        modal_hot = (modality[micro][:, None] == jnp.arange(2, dtype=jnp.int32)[None, :]).astype(jnp.float32)
        counts = counts + jnp.dot(modal_hot.T, onehot, precision=lax.Precision.HIGHEST)
        prob_sums = prob_sums + jnp.dot(modal_hot.T, router_probs, precision=lax.Precision.HIGHEST)
        modal_counts = modal_counts + jnp.sum(modal_hot, axis=0)
    load = jnp.stack([EXPERTS * counts / modal_counts[:, None], EXPERTS * prob_sums / modal_counts[:, None]])
    return jnp.stack(mixed_list), load
```

```python
import functools

import jax
import jax.numpy as jnp
from jax import lax
from jax.experimental import pallas as pl
from jax.experimental.pallas import tpu as pltpu
from jax.sharding import Mesh
from jax.sharding import PartitionSpec as P

EXPERT = ("expert_0", "expert_1")
EXPERT_DP = ("expert_0", "expert_1", "dp_0", "dp_1")
Z = "dp_0"
CORE = "dp_1"
SWAP = [(0, 1), (1, 0)]
CHUNKS = (640, 640)
STAT_LANES = 128
STAT_ROWS = 16
PART = 8


VMEM = pl.BlockSpec(memory_space=pltpu.VMEM)
SMEM = pl.BlockSpec(memory_space=pltpu.SMEM)
ANY = pl.BlockSpec(memory_space=pl.ANY)


def split3(value, narrow):
    high = narrow(value)
    middle = narrow(value - high)
    low = narrow(value - high - middle)
    return high, middle, low


def route_body(tokens, routes, modality, router, buffer, slot_out, gate_out):
    rows, width = tokens.shape
    micros, count = routes.shape
    experts = router.shape[1]
    capacity = 2 * count // experts
    slots = micros * experts * capacity
    logits = lax.dot_general(
        router[...], tokens[...], (((0,), (1,)), ((), ())), preferred_element_type=jnp.float32
    )
    expert_at = lax.broadcasted_iota(jnp.int32, (experts, count), 0)
    earlier = lax.broadcasted_iota(jnp.int32, (count, count), 0) <= lax.broadcasted_iota(
        jnp.int32, (count, count), 1
    )
    earlier = earlier.astype(jnp.bfloat16)
    slot_rows, hots = [], []
    for micro in range(micros):
        route = routes[micro : micro + 1, :]
        hot = (expert_at == route).astype(jnp.float32)
        running = jnp.dot(hot.astype(jnp.bfloat16), earlier, preferred_element_type=jnp.float32)
        place = jnp.sum((running - 1.0) * hot, axis=0, keepdims=True).astype(jnp.int32)
        slot_rows.append((route * micros + micro) * capacity + place)
        hots.append(hot)
    slot = jnp.concatenate(slot_rows, axis=1)
    hot = jnp.concatenate(hots, axis=1)
    slot_out[...] = slot
    own = jnp.sum(logits * hot, axis=0, keepdims=True)
    gating = 1.0 / (1.0 + jnp.exp(-own))
    chosen = lax.broadcasted_iota(jnp.int32, (slots, rows), 0) == slot
    gate_out[...] = jnp.sum(jnp.where(chosen, gating, 0.0), axis=1, keepdims=True)
    placed = jnp.dot(chosen.astype(jnp.bfloat16), tokens[...], preferred_element_type=jnp.float32)
    buffer[:, :width] = placed.astype(jnp.bfloat16)

    exps = jnp.exp(logits)
    probs = exps / jnp.sum(exps, axis=0, keepdims=True)
    text = jnp.concatenate([modality[m : m + 1, :] for m in range(micros)], axis=1)
    lane = lax.broadcasted_iota(jnp.int32, (experts, STAT_LANES), 1)
    stat = jnp.zeros((experts, STAT_LANES), jnp.float32)
    for kind in range(2):
        modal = (text == kind).astype(jnp.float32)
        counts = jnp.sum(hot * modal, axis=1, keepdims=True)
        prob_sums = jnp.sum(probs * modal, axis=1, keepdims=True)
        total = jnp.sum(modal, axis=1, keepdims=True)
        stat = jnp.where(lane % PART == kind, counts, stat)
        stat = jnp.where(lane % PART == 2 + kind, prob_sums, stat)
        stat = jnp.where(lane % PART == 4 + kind, jnp.broadcast_to(total, counts.shape), stat)
    high, middle, low = split3(stat, lambda v: v.astype(jnp.bfloat16).astype(jnp.float32))
    part = lane // PART
    coded = jnp.where(part == 0, high, jnp.where(part == 1, middle, jnp.where(part == 2, low, 0.0)))
    coded = coded.astype(jnp.bfloat16)
    blank = jnp.zeros_like(coded)
    block = jnp.concatenate([coded, blank], axis=0)
    buffer[:, width:] = jnp.concatenate([block] * experts, axis=0)


def route_call(tokens, routes, modality, router):
    rows, width = tokens.shape
    micros, count = routes.shape
    experts = router.shape[1]
    slots = 2 * count * micros
    return pl.pallas_call(
        route_body,
        in_specs=[VMEM] * 4,
        out_specs=[VMEM] * 3,
        out_shape=[
            jax.ShapeDtypeStruct((slots, width + STAT_LANES), jnp.bfloat16),
            jax.ShapeDtypeStruct((1, rows), jnp.int32),
            jax.ShapeDtypeStruct((slots, 1), jnp.float32),
        ],
        compiler_params=pltpu.CompilerParams(vmem_limit_bytes=32 << 20),
        name="route",
    )(tokens, routes, modality, router)


def prepare_body(place, w_in, own, sent):
    core = place[1]
    rows, units = w_in.shape
    width = own.shape[1]
    group = 2 * (width // own_groups(width, units))
    half = group // 2
    even = jnp.concatenate([w_in[:, at : at + half] for at in range(0, units, group)], axis=1)
    odd = jnp.concatenate([w_in[:, at + half : at + group] for at in range(0, units, group)], axis=1)
    first = core == 0
    own[...] = jnp.where(first, even, odd)
    sent[...] = jnp.where(first, odd, even)


def own_groups(width, units):
    return 8


def prepare_call(place, w_in):
    rows, units = w_in.shape
    shape = jax.ShapeDtypeStruct((rows, units // 2), w_in.dtype)
    return pl.pallas_call(
        prepare_body,
        in_specs=[SMEM, VMEM],
        out_specs=[VMEM] * 2,
        out_shape=[shape, shape],
        compiler_params=pltpu.CompilerParams(vmem_limit_bytes=16 << 20),
        name="prepare",
    )(place, w_in)


def load_pieces(place, pieces, spots, whole, sems):
    copies = []
    for index, (piece, spot) in enumerate(zip(pieces, spots)):
        at, size = spot(place[0], place[1])
        target = whole.at[pl.ds(pl.multiple_of(at, 16), size), :]
        copy = pltpu.make_async_copy(piece.at[pl.ds(0, size), :], target, sems.at[index])
        copy.start()
        copies.append(copy)
    return copies


def gelu(v):
    return 0.5 * v * (1.0 + jnp.tanh(0.7978845608028654 * (v + 0.044715 * (v * v * v))))


def first_body(spots, width, block, place, mine, theirs, *rest):
    pieces, (hidden, whole, sems) = rest[: len(spots)], rest[len(spots) :]
    for copy in load_pieces(place, pieces, spots, whole, sems):
        copy.wait()
    slots = mine.shape[0]

    def step(index, _):
        at = pl.multiple_of(index * block, block)
        columns = whole[:, pl.ds(at, block)]
        for start, source in ((0, mine), (slots, theirs)):
            value = jnp.dot(source[:, :width], columns, preferred_element_type=jnp.float32)
            hidden[start : start + slots, pl.ds(at, block)] = gelu(value).astype(jnp.bfloat16)
        return 0

    lax.fori_loop(0, hidden.shape[1] // block, step, 0)


def first_call(place, mine, theirs, pieces, spots, width):
    units = pieces[0].shape[1]
    slots = mine.shape[0]
    return pl.pallas_call(
        functools.partial(first_body, spots, width, 512),
        in_specs=[SMEM, VMEM, VMEM] + [ANY] * len(pieces),
        out_specs=VMEM,
        out_shape=jax.ShapeDtypeStruct((2 * slots, units), jnp.bfloat16),
        scratch_shapes=[
            pltpu.VMEM((width, units), jnp.bfloat16),
            pltpu.SemaphoreType.DMA((len(pieces),)),
        ],
        compiler_params=pltpu.CompilerParams(vmem_limit_bytes=48 << 20),
        cost_estimate=pl.CostEstimate(
            flops=4 * slots * width * units, bytes_accessed=2 * width * units, transcendentals=0
        ),
        name="first",
    )(place, mine, theirs, *pieces)


def second_body(spots, place, hidden, *rest):
    pieces, (own, sent, whole, sems) = rest[: len(spots)], rest[len(spots) :]
    for copy in load_pieces(place, pieces, spots, whole, sems):
        copy.wait()
    slots = own.shape[0]
    sent[...] = jnp.dot(hidden[slots:, :], whole[...], preferred_element_type=jnp.float32).astype(
        jnp.bfloat16
    )
    own[...] = jnp.dot(hidden[:slots, :], whole[...], preferred_element_type=jnp.float32)


def second_call(place, hidden, pieces, spots):
    units = hidden.shape[1]
    slots = hidden.shape[0] // 2
    width = pieces[0].shape[1]
    return pl.pallas_call(
        functools.partial(second_body, spots),
        in_specs=[SMEM, VMEM] + [ANY] * len(pieces),
        out_specs=[VMEM] * 2,
        out_shape=[
            jax.ShapeDtypeStruct((slots, width), jnp.float32),
            jax.ShapeDtypeStruct((slots, width), jnp.bfloat16),
        ],
        scratch_shapes=[
            pltpu.VMEM((units, width), jnp.bfloat16),
            pltpu.SemaphoreType.DMA((len(pieces),)),
        ],
        compiler_params=pltpu.CompilerParams(vmem_limit_bytes=40 << 20),
        cost_estimate=pl.CostEstimate(
            flops=4 * slots * width * units, bytes_accessed=2 * width * units, transcendentals=0
        ),
        name="second",
    )(place, hidden, *pieces)


def combine_body(starts, slot, gate, *rest):
    returned, out = rest[:-1], rest[-1]
    slots = gate.shape[0]
    rows = slot.shape[1]
    chosen = lax.broadcasted_iota(jnp.int32, (slots, rows), 0) == slot[...]
    chosen = chosen.astype(jnp.bfloat16)
    for at, part in zip(starts, returned):
        scaled = (part[...].astype(jnp.float32) * gate[...]).astype(jnp.bfloat16)
        value = lax.dot_general(
            chosen, scaled, (((0,), (0,)), ((), ())), preferred_element_type=jnp.float32
        )
        out[:, at : at + part.shape[1]] = value.astype(jnp.bfloat16)


def combine_call(slot, gate, returned, starts):
    width = sum(part.shape[1] for part in returned)
    return pl.pallas_call(
        functools.partial(combine_body, starts),
        in_specs=[VMEM] * (2 + len(returned)),
        out_specs=VMEM,
        out_shape=jax.ShapeDtypeStruct((slot.shape[1], width), jnp.bfloat16),
        compiler_params=pltpu.CompilerParams(vmem_limit_bytes=16 << 20),
        name="combine",
    )(slot, gate, *returned)


def shift(value, count, by):
    return lax.ppermute(value, Z, [(i, (i + by) % count) for i in range(count)])


def swap_core(value):
    return lax.ppermute(value, CORE, SWAP)


def ring_of_two(first, second, count):
    hops = [[(0, 0, first), (0, 1, second)]]
    first_up = first_down = first
    second_up = second_down = second
    half = count // 2
    for hop in range(1, half + 1):
        first_up = shift(first_up, count, 1)
        second_down = shift(second_down, count, -1)
        arrived = [(-hop, 0, first_up), (hop, 1, second_down)]
        if hop < half:
            second_up = shift(second_up, count, 1)
            first_down = shift(first_down, count, -1)
            arrived += [(-hop, 1, second_up), (hop, 0, first_down)]
        hops.append(arrived)
    return hops


def ring_of_one(piece, count, cut):
    hops = [[(0, None, piece)]]
    up = down = piece
    half = count // 2
    for hop in range(1, half):
        up = shift(up, count, 1)
        down = shift(down, count, -1)
        hops.append([(-hop, None, up), (hop, None, down)])
    upper = shift(up[:cut], count, 1)
    lower = shift(down[cut:], count, -1)
    hops.append([(-half, 0, upper), (half, 1, lower)])
    return hops


def gated(values, hop):
    held = lax.optimization_barrier(tuple(values) + tuple(piece for _, _, piece in hop))
    return held[: len(values)]


def on_device(tokens, modality, routes, router, w_in, w_out, sizes):
    micro_count, tok_count, model_width = tokens.shape
    experts = router.shape[1]
    capacity = 2 * tok_count // experts
    slots = experts * micro_count * capacity
    count = sizes[Z]
    place = jnp.stack([lax.axis_index(Z), lax.axis_index(CORE)]).astype(jnp.int32)
    in_rows = w_in.shape[1]
    out_rows = w_out.shape[1]

    own_piece, sent_piece = prepare_call(place, w_in[0])
    other_piece = swap_core(sent_piece)
    in_hops = ring_of_two(own_piece, other_piece, count)

    buffer, slot, gate = route_call(
        tokens.reshape(micro_count * tok_count, model_width), routes[:, :, 0], modality, router
    )
    buffer = buffer.reshape(experts, micro_count * capacity, -1)
    arrived = lax.all_to_all(buffer, EXPERT, split_axis=0, concat_axis=0, tiled=True)
    theirs = swap_core(arrived)

    def decode(coded):
        parts = coded.astype(jnp.float32)
        return parts[..., 0:PART] + parts[..., PART : 2 * PART] + parts[..., 2 * PART : 3 * PART]

    def narrow(value):
        return lax.reduce_precision(value, 8, 7)

    coded = jnp.concatenate(
        [arrived[:, :STAT_ROWS, model_width:], theirs[:, :STAT_ROWS, model_width:]], axis=0
    )
    stat = jnp.sum(decode(coded), axis=0)
    coded = jnp.concatenate(split3(stat, narrow), axis=1).astype(jnp.bfloat16)
    starts = [sum(CHUNKS[:i]) for i in range(len(CHUNKS))]
    pieces = [w_out[0, :, at : at + width] for at, width in zip(starts, CHUNKS)]
    coded = jnp.pad(coded, ((0, 0), (0, CHUNKS[-1] - coded.shape[1])))
    pieces[-1] = jnp.concatenate([pieces[-1], coded], axis=0)

    cut = out_rows // 2
    out_hops = []
    for index, piece in enumerate(pieces):
        (piece,) = gated([piece], in_hops[2 + index])
        out_hops.append(ring_of_one(piece, count, cut))

    in_pieces = [item for hop in in_hops for item in hop]
    in_spots = [
        functools.partial(
            lambda distance, which, z, core: (
                2 * in_rows * lax.rem(z + distance + count, count)
                + in_rows * (core if which == 0 else 1 - core),
                in_rows,
            ),
            distance,
            which,
        )
        for distance, which, _ in in_pieces
    ]
    hidden = first_call(
        place,
        arrived.reshape(slots, -1),
        theirs.reshape(slots, -1),
        [piece for _, _, piece in in_pieces],
        in_spots,
        model_width,
    )

    returned = []
    for hops in out_hops:
        items = [item for hop in hops for item in hop]
        spots = [
            functools.partial(
                lambda distance, which, z, core: (
                    out_rows * lax.rem(z + distance + count, count) + (cut if which == 1 else 0),
                    out_rows if which is None else cut,
                ),
                distance,
                which,
            )
            for distance, which, _ in items
        ]
        own, sent = second_call(place, hidden, [piece for _, _, piece in items], spots)
        foreign = swap_core(sent)
        served = (own + foreign.astype(jnp.float32)).astype(jnp.bfloat16)
        served = served.reshape(experts, micro_count * capacity, -1)
        back = lax.all_to_all(served, EXPERT, split_axis=0, concat_axis=0, tiled=True)
        returned.append(back.reshape(slots, -1))
    mixed = combine_call(slot, gate, returned, starts).reshape(tokens.shape)

    total = jnp.zeros_like(stat)
    for hop in out_hops[-1]:
        for _, which, piece in hop:
            if which != 0:
                total = total + decode(piece[-STAT_ROWS:, : 3 * PART])
    counts = total[:, 0:2].T
    prob_sums = total[:, 2:4].T
    modal_counts = total[:, 4:6].T
    load = jnp.stack([experts * counts / modal_counts, experts * prob_sums / modal_counts])
    return (mixed, load)


def solution(mesh):
    torus = Mesh(mesh.devices.reshape(4, 4, 8, 2), EXPERT_DP)
    sizes = dict(torus.shape)
    in_specs = (
        P(None, EXPERT_DP, None),
        P(None, EXPERT_DP),
        P(None, EXPERT_DP, None),
        P(),
        P(EXPERT, (Z, CORE), None),
        P(EXPERT, (Z, CORE), None),
    )
    out_specs = (P(None, EXPERT_DP, None), P())

    def body(*args):
        return on_device(*args, sizes)

    return jax.shard_map(body, mesh=torus, in_specs=in_specs, out_specs=out_specs, check_vma=False)
```
